32 devices in a mesh: genes: 32 (over z, y, x, core).
Axes of the slice: x: 2, y: 2, z: 4, core: 2. Of those that a mesh axis runs over, the one named last changes fastest.
Arguments:
- expression: bfloat16 [32768, 1024], P('genes'), may hold values from -10 to 20
- labels: int32 [32768], P('genes'), may hold values from 0 to 399
Outputs:
- membership: float32 [32768, 400], P('genes')
- eigengenes: bfloat16 [400, 1024], replicated
The draws below stay inside these ranges and needn't reach their ends.
All inputs are finite; a program needn't handle non-finite values.
Results may differ from the reference program's by a relative error of at most 0.0012.
The reference program's roundings to bfloat16 on the way (of `standard` and `weights`) count: a program that leaves them out, or rounds other values in their place, can miss the bound.
Values may be sent and summed in bfloat16 or wider, within the bound.
No kernel may reach another device: no remote copies, remote signals or barrier semaphores. Data moves between devices by JAX's collectives and lax.ppermute only.
A program may use at most 64 MiB of HBM per device.

```python
import jax
import jax.numpy as jnp
from jax import lax

SAMPLES = 1024
MODULES = 400
GENES_DEV = 1024
ITERS = 2
GENES = 32768
N_GENES = 32


def draw_expression(key, part):
    draw_key = jax.random.fold_in(key, 11)
    factors = jax.random.normal(jax.random.fold_in(draw_key, 1), (MODULES, SAMPLES), jnp.float32)
    column = jnp.arange(SAMPLES, dtype=jnp.float32) / SAMPLES
    sample_ramp = 1.0 + 2.0 * column
    factors = factors * sample_ramp[None, :]

    def one_block(block_index):
        block_key = jax.random.fold_in(draw_key, block_index + 2)
        key_one, key_two, key_three, key_four = jax.random.split(block_key, 4)
        cluster = jax.random.randint(key_one, (GENES_DEV,), 0, MODULES)
        signal = jnp.take(factors, cluster, axis=0)
        offset = jax.random.uniform(key_four, (GENES_DEV, 1), jnp.float32, 2.0, 8.0)
        loading = jax.random.uniform(key_two, (GENES_DEV, 1), jnp.float32, 0.3, 1.5)
        noise_part = jax.random.normal(key_three, (GENES_DEV, SAMPLES), jnp.float32)
        return jnp.clip(offset + loading * signal + noise_part, -10.0, 20.0)
    blocks = lax.map(one_block, jnp.arange(GENES // GENES_DEV))
    return blocks.reshape(GENES, SAMPLES).astype(jnp.bfloat16)


def touch_ends(result, stream_key, least, high):
    shape = result.shape
    index_at = [jax.random.randint(jax.random.fold_in(stream_key, axis), (), 0, shape[axis]) for axis in range(len(shape))]
    result = result.at[tuple(index_at)].set(least)
    longest = shape.index(max(shape))
    index_at[longest] = (index_at[longest] + 1) % shape[longest]
    return result.at[tuple(index_at)].set(high)


def setup_inputs(seed: int = 0) -> dict:
    splits = jax.random.split(jax.random.key(seed), 3)
    expression = draw_expression(jax.random.fold_in(splits[2], 71), 0)
    labels = touch_ends(jax.random.randint(splits[1], (GENES,), 0, MODULES), jax.random.fold_in(splits[1], 1), 0, MODULES - 1).astype(jnp.int32)
    return dict(expression=expression, labels=labels)


epsilon = 1e-05
sharpness = 30.0

def standardize(expression):
    values = expression.astype(jnp.float32)
    centre = lax.optimization_barrier(jnp.mean(values, axis=1, keepdims=True))
    shifted = values - centre
    spread = lax.optimization_barrier(jnp.mean(shifted * shifted, axis=1, keepdims=True))
    return (shifted * lax.rsqrt(spread + epsilon)).astype(jnp.bfloat16)

def reference(expression, labels):
    blocks = expression.reshape(N_GENES, GENES_DEV, SAMPLES)
    standard = lax.map(standardize, blocks).reshape(GENES, SAMPLES)
    module_ids = jnp.arange(MODULES, dtype=jnp.int32)
    weights = (labels.astype(jnp.int32)[:, None] == module_ids[None, :]).astype(jnp.bfloat16)
    shares = None
    eigengenes = None
    for iteration in range(ITERS):
        module_sums = lax.dot_general(weights, standard, (((0,), (0,)), ((), ())), preferred_element_type=jnp.float32)
        scale = lax.rsqrt(lax.optimization_barrier(jnp.mean(module_sums * module_sums, axis=1, keepdims=True)) + epsilon)
        eigengenes = (module_sums * scale).astype(jnp.bfloat16)
        correlation = lax.dot_general(standard, eigengenes, (((1,), (1,)), ((), ())), preferred_element_type=jnp.float32) / SAMPLES
        raised = jnp.exp(sharpness * correlation)
        shares = raised / lax.optimization_barrier(jnp.sum(raised, axis=1, keepdims=True))
        weights = shares.astype(jnp.bfloat16)
    return (MODULES * shares, eigengenes)
```

```python
import math

import jax
import jax.numpy as jnp
from jax import lax
from jax.sharding import PartitionSpec as P

MODULES = 400
ITERS = 2


epsilon = 1e-05
sharpness = 30.0

AXIS = "genes"
BLOCKS = 8
ROW_TILE = 8
HALF_MAX = 60000.0


def standardize(expression):
    values = expression.astype(jnp.float32)
    centre = jnp.mean(values, axis=1, keepdims=True)
    shifted = values - centre
    spread = jnp.mean(shifted * shifted, axis=1, keepdims=True)
    return (shifted * lax.rsqrt(spread + epsilon)).astype(jnp.bfloat16)


def swap(value, devices, bit):
    return lax.ppermute(value, AXIS, [(i, i ^ bit) for i in range(devices)])


def power_below(limit):
    return 2.0 ** math.floor(math.log2(limit))


def reduce_block(sums, devices, bound, sent):
    half = sums.shape[0] // 2
    rows = half // 4
    chip = sums[:half] + swap(sums[half:], devices, 1)
    bound = 2.0 * bound
    down = power_below(HALF_MAX / bound)
    others = [
        swap((chip[k * rows:(k + 1) * rows] * down).astype(sent), devices, 2 * k)
        for k in range(1, 4)
    ]
    others = [other.astype(jnp.float32) for other in others]
    total = ((chip[:rows] * down + others[0]) + (others[1] + others[2])) * (1.0 / down)
    bound = 4.0 * bound
    bit = 8
    while bit < devices:
        steps = range(1, min(4, devices // bit))
        down = power_below(HALF_MAX / bound)
        own = (total * down).astype(sent)
        others = [swap(own, devices, bit * k).astype(jnp.float32) for k in steps]
        total = own.astype(jnp.float32) + others[0]
        if len(others) == 3:
            total = total + (others[1] + others[2])
        total = total * (1.0 / down)
        bound = bound * (len(others) + 1)
        bit = bit * (len(others) + 1)
    return total


def gather_blocks(block, devices):
    half = jnp.concatenate([block] + [swap(block, devices, 2 * k) for k in range(1, 4)], axis=0)
    return jnp.concatenate([half, swap(half, devices, 1)], axis=0)


def shards(devices):
    def body(expression, labels):
        genes, samples = expression.shape
        used = -(-MODULES // BLOCKS)
        rows = -(-used // ROW_TILE) * ROW_TILE
        place = lax.axis_index(AXIS)
        mine = (place & 1) * 4 + ((place >> 1) & 3)
        bound = genes * math.sqrt(samples) * 1.02

        standard = standardize(expression)
        column = jnp.arange(BLOCKS * rows, dtype=jnp.int32)
        slot = ((labels // used) ^ mine) * rows + labels % used
        weights = (slot[:, None] == column[None, :]).astype(jnp.bfloat16)
        for iteration in range(ITERS):
            partial_value = lax.dot_general(
                weights, standard, (((0,), (0,)), ((), ())), preferred_element_type=jnp.float32
            )
            total = reduce_block(partial_value, devices, bound, jnp.float16 if iteration == ITERS - 1 else jnp.float32)
            scale = lax.rsqrt(jnp.mean(total * total, axis=1, keepdims=True) + epsilon)
            block = (total * scale).astype(jnp.bfloat16)
            eigengenes = gather_blocks(block, devices)
            last = iteration == ITERS - 1
            if last:
                blocks = eigengenes.reshape(BLOCKS, rows, samples)[:, :used]
                for bit in (4, 2, 1):
                    pairs = blocks.reshape(BLOCKS // (2 * bit), 2, bit, used, samples)
                    blocks = jnp.where((mine & bit) != 0, pairs[:, ::-1], pairs)
                eigengenes = blocks.reshape(BLOCKS * used, samples)[:MODULES]
            correlation = (
                lax.dot_general(
                    standard, eigengenes, (((1,), (1,)), ((), ())), preferred_element_type=jnp.float32
                )
                / samples
            )
            raised = jnp.exp(sharpness * correlation)
            if not last:
                block_of = column // rows
                number = (block_of ^ mine) * used + column % rows
                real = (column % rows < used) & (number < MODULES)
                raised = jnp.where(real[None, :], raised, 0.0)
            shares = raised / jnp.sum(raised, axis=1, keepdims=True)
            weights = shares.astype(jnp.bfloat16)
        return (MODULES * shares, eigengenes)

    return body


def solution(mesh):
    placed = (P(AXIS, None), P(AXIS))
    return jax.shard_map(
        shards(mesh.shape[AXIS]), mesh=mesh, in_specs=placed, out_specs=(P(AXIS, None), P()), check_vma=False
    )
```

```python
import math

import jax
import jax.numpy as jnp
from jax import lax
from jax.experimental import pallas as pl
from jax.experimental.pallas import tpu as pltpu
from jax.sharding import PartitionSpec as P

MODULES = 400
ITERS = 2


epsilon = 1e-05
sharpness = 30.0

AXIS = "genes"
BLOCKS = 8
ROW_TILE = 8
HALF_MAX = 60000.0


def swap(value, devices, bit):
    return lax.ppermute(value, AXIS, [(i, i ^ bit) for i in range(devices)])


def power_below(limit):
    return 2.0 ** math.floor(math.log2(limit))


def to_half(bound):
    down = power_below(HALF_MAX / bound)

    def encode(value):
        return (value * down).astype(jnp.float16)

    def decode(sent):
        return sent.astype(jnp.float32) * (1.0 / down)

    return encode, decode


def normalise(total):
    scale = lax.rsqrt(jnp.mean(total * total, axis=1, keepdims=True) + epsilon)
    return (total * scale).astype(jnp.bfloat16)


def four_sum(own, others):
    total = own + others[0]
    return total + (others[1] + others[2]) if len(others) == 3 else total


def spread(sent, devices, bit):
    steps = range(1, min(4, devices // bit))
    return [swap(sent, devices, bit * k) for k in steps]


def in_plane(kept, given, devices, encode, decode):
    rows = kept.shape[0] // 4
    kept, received = lax.optimization_barrier((kept, swap(given, devices, 1)))
    chip = kept + received
    others = [decode(swap(encode(chip[k * rows:(k + 1) * rows]), devices, 2 * k)) for k in range(1, 4)]
    return four_sum(chip[:rows], others)


def half_block(kept, given, devices, bound):
    total = in_plane(kept, given, devices, *to_half(2.0 * bound))
    bound = 8.0 * bound
    bit = 8
    while bit < devices:
        encode, decode = to_half(bound)
        sent = encode(total)
        others = spread(sent, devices, bit)
        total = four_sum(decode(sent), [decode(other) for other in others])
        bound = bound * (len(others) + 1)
        bit = bit * (len(others) + 1)
    return normalise(total)


def full_block(kept, given, devices, used):
    total = in_plane(kept, given, devices, lambda value: value, lambda value: value)
    rows, samples = total.shape
    bit = 8
    members = min(4, devices // bit)
    if members < 2:
        return normalise(total)
    part = -(-used // members)
    member = (lax.axis_index(AXIS) // bit) % members
    lanes = 128
    parts = jnp.pad(total, ((0, max(0, part * members - rows)), (0, 0)))[:part * members]
    parts = parts.reshape(members, part, samples // lanes, lanes)

    def part_of(k):
        return lax.dynamic_index_in_dim(parts, member ^ k, 0, keepdims=False)

    total = four_sum(part_of(0), [swap(part_of(k), devices, bit * k) for k in range(1, members)])
    rest = bit * members
    while rest < devices:
        others = spread(total, devices, rest)
        total = four_sum(total, others)
        rest = rest * (len(others) + 1)
    scale = lax.rsqrt(jnp.sum(total * total, axis=(1, 2), keepdims=True) * (1.0 / samples) + epsilon)
    mine = (total * scale).astype(jnp.bfloat16)
    pieces = jnp.stack([mine] + spread(mine, devices, bit))
    ordered = [lax.dynamic_index_in_dim(pieces, member ^ m, 0, keepdims=False) for m in range(members)]
    block = jnp.concatenate(ordered, axis=0)[:rows].reshape(-1, samples)
    return jnp.pad(block, ((0, rows - block.shape[0]), (0, 0)))


def gather_blocks(block, devices):
    half = jnp.concatenate([block] + [swap(block, devices, 2 * k) for k in range(1, 4)], axis=0)
    return half, swap(half, devices, 1)


CHUNKS = 4
KERNEL_BYTES = 24 << 20


def dot_tt(a, b):
    return lax.dot_general(a, b, (((1,), (1,)), ((), ())), preferred_element_type=jnp.float32)


def dot(a, b):
    return lax.dot_general(a, b, (((1,), (0,)), ((), ())), preferred_element_type=jnp.float32)


def slots(label, mine, rows):
    used = -(-MODULES // BLOCKS)
    block = jnp.zeros_like(label)
    for b in range(1, BLOCKS):
        block += jnp.where(label >= b * used, 1, 0)
    return (block ^ mine) * rows + (label - block * used)


def first_kernel(mine_ref, label_ref, expression_ref, standard_ref, given_ref, buffer, sems):
    genes, samples = standard_ref.shape
    size = genes // CHUNKS
    copies = [
        pltpu.make_async_copy(expression_ref.at[pl.ds(c * size, size)], buffer.at[pl.ds(c * size, size)], sems.at[c])
        for c in range(CHUNKS)
    ]
    for copy in copies:
        copy.start()
    slot = slots(label_ref[...], mine_ref[0], given_ref.shape[0] // (BLOCKS // 2)) - given_ref.shape[0]
    for c, copy in enumerate(copies):
        copy.wait()
        span = pl.ds(c * size, size)
        values = buffer[span, :].astype(jnp.float32)
        centre = jnp.sum(values, axis=1, keepdims=True) * (1.0 / samples)
        shifted = values - centre
        spread = jnp.sum(shifted * shifted, axis=1, keepdims=True) * (1.0 / samples)
        part = (shifted * lax.rsqrt(spread + epsilon)).astype(jnp.bfloat16)
        standard_ref[span, :] = part
        row = lax.broadcasted_iota(jnp.int32, (given_ref.shape[0], size), 0)
        weights = jnp.where(row == slot[:, c * size:(c + 1) * size], 1.0, 0.0).astype(jnp.bfloat16)
        if c == 0:
            given_ref[...] = dot(weights, part)
        else:
            given_ref[...] += dot(weights, part)


def raise_half(eigengenes, standard, start, mine):
    samples = standard.shape[1]
    rows = eigengenes.shape[0] // (BLOCKS // 2)
    used = -(-MODULES // BLOCKS)
    row = jnp.arange(eigengenes.shape[0], dtype=jnp.int32)
    number = ((start + row // rows) ^ mine) * used + row % rows
    real = (row % rows < used) & (number < MODULES)
    raised = jnp.exp(dot_tt(standard, eigengenes) * (sharpness / samples))
    return jnp.where(real[None, :], raised, 0.0)


def weigh(weights, standard):
    return lax.dot_general(weights, standard, (((0,), (0,)), ((), ())), preferred_element_type=jnp.float32)


def last_kernel(source_ref, mine_ref, other_ref, standard_ref, share_ref, eigen_ref):
    @pl.when(pl.program_id(0) == 0)
    def _():
        half = mine_ref.shape[0]
        column = lax.broadcasted_iota(jnp.int32, (MODULES, half), 1)
        rows = source_ref[...]
        first = jnp.where(column == rows, 1.0, 0.0).astype(jnp.bfloat16)
        second = jnp.where(column == rows - half, 1.0, 0.0).astype(jnp.bfloat16)
        picked = dot(first, mine_ref[...]) + dot(second, other_ref[...])
        eigen_ref[...] = picked.astype(jnp.bfloat16)

    genes, samples = standard_ref.shape
    size = genes // CHUNKS
    part = standard_ref[pl.ds(pl.multiple_of(pl.program_id(0) * size, size), size), :]
    raised = jnp.exp(dot_tt(eigen_ref[...], part) * (sharpness / samples))
    share_ref[...] = raised * (MODULES / jnp.sum(raised, axis=0, keepdims=True))


def on_chip(value):
    return pltpu.with_memory_space_constraint(value, pltpu.VMEM)


def in_vmem(count):
    return [pl.BlockSpec(memory_space=pltpu.VMEM)] * count


def shards(devices):
    def body(expression, labels):
        genes, samples = expression.shape
        used = -(-MODULES // BLOCKS)
        rows = -(-used // ROW_TILE) * ROW_TILE
        half = BLOCKS // 2 * rows
        place = lax.axis_index(AXIS)
        mine = ((place & 1) * 4 + ((place >> 1) & 3)).astype(jnp.int32)
        bound = genes * math.sqrt(samples) * 1.02
        f32 = jnp.float32

        module = jnp.arange(MODULES, dtype=jnp.int32)
        source = ((module // used) ^ mine) * rows + module % used

        standard, given = pl.pallas_call(
            first_kernel,
            out_shape=[pltpu.VMEM((genes, samples), jnp.bfloat16), pltpu.VMEM((half, samples), f32)],
            in_specs=[
                pl.BlockSpec(memory_space=pltpu.SMEM),
                pl.BlockSpec(memory_space=pltpu.VMEM),
                pl.BlockSpec(memory_space=pltpu.HBM),
            ],
            out_specs=in_vmem(2),
            scratch_shapes=[pltpu.VMEM((genes, samples), jnp.bfloat16), pltpu.SemaphoreType.DMA((CHUNKS,))],
            name="first",
                compiler_params=pltpu.CompilerParams(vmem_limit_bytes=KERNEL_BYTES),
        )(mine[None], labels[None, :], pltpu.with_memory_space_constraint(expression, pltpu.HBM))
        slot = slots(labels, mine, rows)
        column = jnp.arange(half, dtype=jnp.int32)
        kept = weigh((slot[:, None] == column[None, :]).astype(jnp.bfloat16), standard)
        for iteration in range(ITERS):
            last = iteration == ITERS - 1
            block = half_block(kept, given, devices, bound) if last else full_block(kept, given, devices, used)
            own, other = gather_blocks(block, devices)
            if not last:
                mine_raised = raise_half(own, standard, 0, mine)
                other_raised = raise_half(other, standard, BLOCKS // 2, mine)
                total = jnp.sum(mine_raised, axis=1, keepdims=True) + jnp.sum(other_raised, axis=1, keepdims=True)
                given = weigh((other_raised / total).astype(jnp.bfloat16), standard)
                kept = weigh((mine_raised / total).astype(jnp.bfloat16), standard)
        size = genes // CHUNKS
        shares, eigengenes = pl.pallas_call(
            last_kernel,
            out_shape=[
                jax.ShapeDtypeStruct((MODULES, genes), f32),
                jax.ShapeDtypeStruct((MODULES, samples), jnp.bfloat16),
            ],
            grid=(CHUNKS,),
            in_specs=[
                pl.BlockSpec((MODULES, 1), lambda c: (0, 0)),
            ] + in_vmem(3),
            out_specs=[
                pl.BlockSpec((MODULES, size), lambda c: (0, c)),
                pl.BlockSpec((MODULES, samples), lambda c: (0, 0)),
            ],
            name="last",
                compiler_params=pltpu.CompilerParams(vmem_limit_bytes=KERNEL_BYTES),
        )(source[:, None], on_chip(own), on_chip(other), on_chip(standard))
        return shares.T, eigengenes

    return body


def solution(mesh):
    placed = (P(AXIS, None), P(AXIS))
    return jax.shard_map(
        shards(mesh.shape[AXIS]), mesh=mesh, in_specs=placed, out_specs=(P(AXIS, None), P()), check_vma=False
    )
```

```python
import math

import jax
import jax.numpy as jnp
from jax import lax
from jax.experimental import pallas as pl
from jax.experimental.pallas import tpu as pltpu
from jax.sharding import PartitionSpec as P

MODULES = 400
ITERS = 2


epsilon = 1e-05
sharpness = 30.0

AXIS = "genes"
BLOCKS = 8
ROW_TILE = 8
HALF_MAX = 60000.0


def swap(value, devices, bit):
    return lax.ppermute(value, AXIS, [(i, i ^ bit) for i in range(devices)])


def power_below(limit):
    return 2.0 ** math.floor(math.log2(limit))


def to_half(bound):
    down = power_below(HALF_MAX / bound)

    def encode(value):
        return (value * down).astype(jnp.float16)

    def decode(sent):
        return sent.astype(jnp.float32) * (1.0 / down)

    return encode, decode


EXTRA = 2
PER_WORD = 16 // EXTRA
PIECES = 3
LOWEST = -28
SHIFT = 15 + EXTRA
LANES = 128


def power_of_two(number, sign):
    power = jnp.ones(number.shape, jnp.float32)
    for bit in range(6):
        power = power * jnp.where((number >> bit) & 1 == 1, 2.0 ** (sign * (1 << bit)), 1.0)
    return power


def words_for(tiles):
    return -(-(tiles + 1) // PER_WORD)


def encode_fixed(value, out_ref):
    rows, width = value.shape
    tiles = rows // ROW_TILE
    largest = jnp.max(jnp.abs(value), axis=1, keepdims=True)
    exponent = jnp.ceil(jnp.log2(jnp.maximum(largest, 2.0 ** LOWEST) * 1.001))
    exponent = jnp.clip(exponent.astype(jnp.int32) - LOWEST, 0, 63)
    inverse = power_of_two(exponent, -1) * 2.0 ** (SHIFT - LOWEST)
    whole = jnp.clip(jnp.round(value * inverse), -(2.0 ** SHIFT), 2.0 ** SHIFT - 1.0)
    number = whole.astype(jnp.int32)
    lower = number & ((1 << EXTRA) - 1)
    lane = lax.broadcasted_iota(jnp.int32, (ROW_TILE, width), 1)
    marked = jnp.zeros((ROW_TILE, width), jnp.int32)
    for t in range(tiles):
        scale = exponent[t * ROW_TILE:(t + 1) * ROW_TILE]
        for i in range(PIECES):
            piece = (scale >> (EXTRA * i)) & ((1 << EXTRA) - 1)
            marked = jnp.where(lane == PIECES * t + i, piece, marked)
    slots = [lower[t * ROW_TILE:(t + 1) * ROW_TILE] for t in range(tiles)] + [marked]
    packed = []
    for w in range(words_for(tiles)):
        word = jnp.full((ROW_TILE, width), -(1 << 15), jnp.int32)
        for i, slot in enumerate(slots[w * PER_WORD:(w + 1) * PER_WORD]):
            word = word + (slot << (EXTRA * i))
        packed.append(word)
    out_ref[...] = jnp.concatenate([number >> EXTRA] + packed, axis=0).astype(jnp.int16)
    return whole * (power_of_two(exponent, 1) * 2.0 ** (LOWEST - SHIFT))


def decode_fixed(ref, rows):
    tiles = rows // ROW_TILE
    sent = ref[...].astype(jnp.int32)
    packed = [
        sent[rows + w * ROW_TILE:rows + (w + 1) * ROW_TILE] + (1 << 15) for w in range(words_for(tiles))
    ]
    slots = [(packed[t // PER_WORD] >> (EXTRA * (t % PER_WORD))) & ((1 << EXTRA) - 1) for t in range(tiles + 1)]
    number = (sent[:rows] << EXTRA) + jnp.concatenate(slots[:tiles], axis=0)
    marked = slots[tiles][:, :LANES].astype(jnp.float32)
    lane = lax.broadcasted_iota(jnp.int32, (ROW_TILE, LANES), 1)
    exponents = []
    for t in range(tiles):
        scale = jnp.zeros((ROW_TILE, LANES), jnp.float32)
        for i in range(PIECES):
            scale = jnp.where(lane == PIECES * t + i, marked * float(1 << (EXTRA * i)), scale)
        exponents.append(jnp.sum(scale, axis=1, keepdims=True))
    exponent = jnp.concatenate(exponents, axis=0).astype(jnp.int32)
    unit = power_of_two(exponent, 1) * 2.0 ** (LOWEST - SHIFT)
    return number.astype(jnp.float32) * unit


def encode_kernel(kept_ref, received_ref, own_ref, *out_refs):
    rows = own_ref.shape[0]
    own_ref[...] = kept_ref[pl.ds(0, rows), :] + received_ref[pl.ds(0, rows), :]
    for k, out_ref in enumerate(out_refs):
        span = pl.ds((k + 1) * rows, rows)
        encode_fixed(kept_ref[span, :] + received_ref[span, :], out_ref)


def sum_received(own_ref, refs):
    return four_sum(own_ref[...], [decode_fixed(ref, own_ref.shape[0]) for ref in refs])


def recode_kernel(own_ref, *refs):
    refs, (total_ref, out_ref) = refs[:-2], refs[-2:]
    total_ref[...] = encode_fixed(sum_received(own_ref, refs), out_ref)


def finish_kernel(own_ref, *refs):
    refs[-1][...] = normalise(sum_received(own_ref, refs[:-1]))


def normalise(total):
    scale = lax.rsqrt(jnp.mean(total * total, axis=1, keepdims=True) + epsilon)
    return (total * scale).astype(jnp.bfloat16)


def four_sum(own, others):
    total = own + others[0]
    return total + (others[1] + others[2]) if len(others) == 3 else total


def spread(sent, devices, bit):
    steps = range(1, min(4, devices // bit))
    return [swap(sent, devices, bit * k) for k in steps]


def across_cores(kept, given, devices):
    return lax.optimization_barrier((kept, swap(given, devices, 1)))


def half_block(kept, given, devices, bound):
    kept, received = across_cores(kept, given, devices)
    chip = kept + received
    rows = kept.shape[0] // 4
    encode, decode = to_half(2.0 * bound)
    others = [decode(swap(encode(chip[k * rows:(k + 1) * rows]), devices, 2 * k)) for k in range(1, 4)]
    total = four_sum(chip[:rows], others)
    bound = 8.0 * bound
    bit = 8
    while bit < devices:
        encode, decode = to_half(bound)
        sent = encode(total)
        others = spread(sent, devices, bit)
        total = four_sum(decode(sent), [decode(other) for other in others])
        bound = bound * (len(others) + 1)
        bit = bit * (len(others) + 1)
    return normalise(total)


def full_block(kept, given, devices):
    kept, received = across_cores(kept, given, devices)
    rows, samples = kept.shape[0] // 4, kept.shape[1]
    own = pltpu.VMEM((rows, samples), jnp.float32)
    coded = pltpu.VMEM((rows + ROW_TILE * words_for(rows // ROW_TILE), samples), jnp.int16)

    def call(kernel, out_shape, *operands):
        return pl.pallas_call(
            kernel,
            out_shape=out_shape,
            in_specs=in_vmem(len(operands)),
            out_specs=in_vmem(len(out_shape)),
            compiler_params=pltpu.CompilerParams(vmem_limit_bytes=KERNEL_BYTES),
        )(*[on_chip(operand) for operand in operands])

    total, *sent = call(encode_kernel, [own] + [coded] * 3, kept, received)
    others = [swap(sent[k - 1], devices, 2 * k) for k in range(1, 4)]
    bit = 8
    while bit < devices:
        total, sent = call(recode_kernel, [own, coded], total, *others)
        others = spread(sent, devices, bit)
        bit = bit * (len(others) + 1)
    return call(finish_kernel, [pltpu.VMEM((rows, samples), jnp.bfloat16)], total, *others)[0]


def gather_blocks(block, devices):
    half = jnp.concatenate([block] + [swap(block, devices, 2 * k) for k in range(1, 4)], axis=0)
    return half, swap(half, devices, 1)


CHUNKS = 4
KERNEL_BYTES = 24 << 20


def dot_tt(a, b):
    return lax.dot_general(a, b, (((1,), (1,)), ((), ())), preferred_element_type=jnp.float32)


def dot(a, b):
    return lax.dot_general(a, b, (((1,), (0,)), ((), ())), preferred_element_type=jnp.float32)


def slots(label, mine, rows):
    used = -(-MODULES // BLOCKS)
    block = jnp.zeros_like(label)
    for b in range(1, BLOCKS):
        block += jnp.where(label >= b * used, 1, 0)
    return (block ^ mine) * rows + (label - block * used)


def first_kernel(mine_ref, label_hbm, expression_ref, standard_ref, given_ref, buffer, label_ref, sems, label_sem):
    genes, samples = standard_ref.shape
    size = genes // CHUNKS
    copies = [
        pltpu.make_async_copy(expression_ref.at[pl.ds(c * size, size)], buffer.at[pl.ds(c * size, size)], sems.at[c])
        for c in range(CHUNKS)
    ]
    label_copy = pltpu.make_async_copy(label_hbm, label_ref, label_sem)
    label_copy.start()
    for copy in copies:
        copy.start()
    label_copy.wait()
    slot = slots(label_ref[...], mine_ref[0], given_ref.shape[0] // (BLOCKS // 2)) - given_ref.shape[0]
    for c, copy in enumerate(copies):
        copy.wait()
        span = pl.ds(c * size, size)
        values = buffer[span, :].astype(jnp.float32)
        centre = jnp.sum(values, axis=1, keepdims=True) * (1.0 / samples)
        shifted = values - centre
        spread = jnp.sum(shifted * shifted, axis=1, keepdims=True) * (1.0 / samples)
        part = (shifted * lax.rsqrt(spread + epsilon)).astype(jnp.bfloat16)
        standard_ref[span, :] = part
        row = lax.broadcasted_iota(jnp.int32, (given_ref.shape[0], size), 0)
        weights = jnp.where(row == slot[:, c * size:(c + 1) * size], 1.0, 0.0).astype(jnp.bfloat16)
        if c == 0:
            given_ref[...] = dot(weights, part)
        else:
            given_ref[...] += dot(weights, part)


def raise_half(eigengenes, standard, start, mine):
    samples = standard.shape[1]
    rows = eigengenes.shape[0] // (BLOCKS // 2)
    used = -(-MODULES // BLOCKS)
    row = jnp.arange(eigengenes.shape[0], dtype=jnp.int32)
    number = ((start + row // rows) ^ mine) * used + row % rows
    real = (row % rows < used) & (number < MODULES)
    raised = jnp.exp(dot_tt(standard, eigengenes) * (sharpness / samples))
    return jnp.where(real[None, :], raised, 0.0)


def weigh(weights, standard):
    return lax.dot_general(weights, standard, (((0,), (0,)), ((), ())), preferred_element_type=jnp.float32)


def last_kernel(source_ref, mine_ref, other_ref, standard_ref, share_ref, eigen_ref):
    @pl.when(pl.program_id(0) == 0)
    def _():
        half = mine_ref.shape[0]
        column = lax.broadcasted_iota(jnp.int32, (MODULES, half), 1)
        rows = source_ref[...]
        first = jnp.where(column == rows, 1.0, 0.0).astype(jnp.bfloat16)
        second = jnp.where(column == rows - half, 1.0, 0.0).astype(jnp.bfloat16)
        picked = dot(first, mine_ref[...]) + dot(second, other_ref[...])
        eigen_ref[...] = picked.astype(jnp.bfloat16)

    genes, samples = standard_ref.shape
    size = genes // CHUNKS
    part = standard_ref[pl.ds(pl.multiple_of(pl.program_id(0) * size, size), size), :]
    raised = jnp.exp(dot_tt(eigen_ref[...], part) * (sharpness / samples))
    share_ref[...] = raised * (MODULES / jnp.sum(raised, axis=0, keepdims=True))


def on_chip(value):
    return pltpu.with_memory_space_constraint(value, pltpu.VMEM)


def in_vmem(count):
    return [pl.BlockSpec(memory_space=pltpu.VMEM)] * count


def shards(devices):
    def body(expression, labels):
        genes, samples = expression.shape
        used = -(-MODULES // BLOCKS)
        rows = -(-used // ROW_TILE) * ROW_TILE
        half = BLOCKS // 2 * rows
        place = lax.axis_index(AXIS)
        mine = ((place & 1) * 4 + ((place >> 1) & 3)).astype(jnp.int32)
        bound = genes * math.sqrt(samples) * 1.02
        f32 = jnp.float32

        module = jnp.arange(MODULES, dtype=jnp.int32)
        source = ((module // used) ^ mine) * rows + module % used

        standard, given = pl.pallas_call(
            first_kernel,
            out_shape=[pltpu.VMEM((genes, samples), jnp.bfloat16), pltpu.VMEM((half, samples), f32)],
            in_specs=[
                pl.BlockSpec(memory_space=pltpu.SMEM),
                pl.BlockSpec(memory_space=pltpu.HBM),
                pl.BlockSpec(memory_space=pltpu.HBM),
            ],
            out_specs=in_vmem(2),
            scratch_shapes=[
                pltpu.VMEM((genes, samples), jnp.bfloat16),
                pltpu.VMEM((1, genes), jnp.int32),
                pltpu.SemaphoreType.DMA((CHUNKS,)),
                pltpu.SemaphoreType.DMA,
            ],
            name="first",
                compiler_params=pltpu.CompilerParams(vmem_limit_bytes=KERNEL_BYTES),
        )(mine[None], pltpu.with_memory_space_constraint(labels[None, :], pltpu.HBM), pltpu.with_memory_space_constraint(expression, pltpu.HBM))
        slot = slots(labels, mine, rows)
        column = jnp.arange(half, dtype=jnp.int32)
        kept = weigh((slot[:, None] == column[None, :]).astype(jnp.bfloat16), standard)
        for iteration in range(ITERS):
            last = iteration == ITERS - 1
            block = half_block(kept, given, devices, bound) if last else full_block(kept, given, devices)
            own, other = gather_blocks(block, devices)
            if not last:
                mine_raised = raise_half(own, standard, 0, mine)
                other_raised = raise_half(other, standard, BLOCKS // 2, mine)
                total = jnp.sum(mine_raised, axis=1, keepdims=True) + jnp.sum(other_raised, axis=1, keepdims=True)
                given = weigh((other_raised / total).astype(jnp.bfloat16), standard)
                kept = weigh((mine_raised / total).astype(jnp.bfloat16), standard)
        size = genes // CHUNKS
        shares, eigengenes = pl.pallas_call(
            last_kernel,
            out_shape=[
                jax.ShapeDtypeStruct((MODULES, genes), f32),
                jax.ShapeDtypeStruct((MODULES, samples), jnp.bfloat16),
            ],
            grid=(CHUNKS,),
            in_specs=[
                pl.BlockSpec((MODULES, 1), lambda c: (0, 0)),
            ] + in_vmem(3),
            out_specs=[
                pl.BlockSpec((MODULES, size), lambda c: (0, c)),
                pl.BlockSpec((MODULES, samples), lambda c: (0, 0)),
            ],
            name="last",
                compiler_params=pltpu.CompilerParams(vmem_limit_bytes=KERNEL_BYTES),
        )(source[:, None], on_chip(own), on_chip(other), on_chip(standard))
        return shares.T, eigengenes

    return body


def solution(mesh):
    placed = (P(AXIS, None), P(AXIS))
    return jax.shard_map(
        shards(mesh.shape[AXIS]), mesh=mesh, in_specs=placed, out_specs=(P(AXIS, None), P()), check_vma=False
    )
```

```python
import math

import jax
import jax.numpy as jnp
from jax import lax
from jax.experimental import pallas as pl
from jax.experimental.pallas import tpu as pltpu
from jax.sharding import PartitionSpec as P


MODULES = 400
ITERS = 2


epsilon = 1e-05
sharpness = 30.0

AXIS = "genes"
BLOCKS = 8
ROW_TILE = 8
HALF_MAX = 60000.0


def swap(value, devices, bit):
    return lax.ppermute(value, AXIS, [(i, i ^ bit) for i in range(devices)])


def power_below(limit):
    return 2.0 ** math.floor(math.log2(limit))


def to_half(bound):
    down = power_below(HALF_MAX / bound)

    def encode(value):
        return (value * down).astype(jnp.float16)

    def decode(sent):
        return sent.astype(jnp.float32) * (1.0 / down)

    return encode, decode


EXTRA = 2
PER_WORD = 16 // EXTRA
PIECES = 3
LOWEST = -28
SHIFT = 15 + EXTRA
LANES = 128


def power_of_two(number, sign):
    power = jnp.ones(number.shape, jnp.float32)
    for bit in range(6):
        power = power * jnp.where((number >> bit) & 1 == 1, 2.0 ** (sign * (1 << bit)), 1.0)
    return power


def words_for(tiles):
    return -(-(tiles + 1) // PER_WORD)


def encode_fixed(value, out_ref):
    rows, width = value.shape
    tiles = rows // ROW_TILE
    largest = jnp.max(jnp.abs(value), axis=1, keepdims=True)
    exponent = jnp.ceil(jnp.log2(jnp.maximum(largest, 2.0 ** LOWEST) * 1.001))
    exponent = jnp.clip(exponent.astype(jnp.int32) - LOWEST, 0, 63)
    inverse = power_of_two(exponent, -1) * 2.0 ** (SHIFT - LOWEST)
    whole = jnp.clip(jnp.round(value * inverse), -(2.0 ** SHIFT), 2.0 ** SHIFT - 1.0)
    number = whole.astype(jnp.int32)
    lower = number & ((1 << EXTRA) - 1)
    lane = lax.broadcasted_iota(jnp.int32, (ROW_TILE, width), 1)
    marked = jnp.zeros((ROW_TILE, width), jnp.int32)
    for t in range(tiles):
        scale = exponent[t * ROW_TILE:(t + 1) * ROW_TILE]
        for i in range(PIECES):
            piece = (scale >> (EXTRA * i)) & ((1 << EXTRA) - 1)
            marked = jnp.where(lane == PIECES * t + i, piece, marked)
    slots = [lower[t * ROW_TILE:(t + 1) * ROW_TILE] for t in range(tiles)] + [marked]
    packed = []
    for w in range(words_for(tiles)):
        word = jnp.full((ROW_TILE, width), -(1 << 15), jnp.int32)
        for i, slot in enumerate(slots[w * PER_WORD:(w + 1) * PER_WORD]):
            word = word + (slot << (EXTRA * i))
        packed.append(word)
    out_ref[...] = jnp.concatenate([number >> EXTRA] + packed, axis=0).astype(jnp.int16)
    return whole * (power_of_two(exponent, 1) * 2.0 ** (LOWEST - SHIFT))


def decode_fixed(ref, rows):
    tiles = rows // ROW_TILE
    sent = ref[...].astype(jnp.int32)
    packed = [
        sent[rows + w * ROW_TILE:rows + (w + 1) * ROW_TILE] + (1 << 15) for w in range(words_for(tiles))
    ]
    slots = [(packed[t // PER_WORD] >> (EXTRA * (t % PER_WORD))) & ((1 << EXTRA) - 1) for t in range(tiles + 1)]
    number = (sent[:rows] << EXTRA) + jnp.concatenate(slots[:tiles], axis=0)
    marked = slots[tiles][:, :LANES].astype(jnp.float32)
    lane = lax.broadcasted_iota(jnp.int32, (ROW_TILE, LANES), 1)
    exponents = []
    for t in range(tiles):
        scale = jnp.zeros((ROW_TILE, LANES), jnp.float32)
        for i in range(PIECES):
            scale = jnp.where(lane == PIECES * t + i, marked * float(1 << (EXTRA * i)), scale)
        exponents.append(jnp.sum(scale, axis=1, keepdims=True))
    exponent = jnp.concatenate(exponents, axis=0).astype(jnp.int32)
    unit = power_of_two(exponent, 1) * 2.0 ** (LOWEST - SHIFT)
    return number.astype(jnp.float32) * unit


def encode_kernel(kept_ref, received_ref, own_ref, *out_refs):
    rows = own_ref.shape[0]
    own_ref[...] = kept_ref[pl.ds(0, rows), :] + received_ref[pl.ds(0, rows), :]
    for k, out_ref in enumerate(out_refs):
        span = pl.ds((k + 1) * rows, rows)
        encode_fixed(kept_ref[span, :] + received_ref[span, :], out_ref)


def sum_received(own_ref, refs):
    return four_sum(own_ref[...], [decode_fixed(ref, own_ref.shape[0]) for ref in refs])


def recode_kernel(own_ref, *refs):
    refs, (total_ref, out_ref) = refs[:-2], refs[-2:]
    total_ref[...] = encode_fixed(sum_received(own_ref, refs), out_ref)


def finish_kernel(own_ref, *refs):
    refs[-1][...] = normalise(sum_received(own_ref, refs[:-1]))


def normalise(total):
    scale = lax.rsqrt(jnp.mean(total * total, axis=1, keepdims=True) + epsilon)
    return (total * scale).astype(jnp.bfloat16)


def four_sum(own, others):
    total = own + others[0]
    return total + (others[1] + others[2]) if len(others) == 3 else total


def spread(sent, devices, bit):
    steps = range(1, min(4, devices // bit))
    return [swap(sent, devices, bit * k) for k in steps]


def across_cores(kept, given, devices):
    return lax.optimization_barrier((kept, swap(given, devices, 1)))


def cuts(rows):
    first = rows // (2 * ROW_TILE) * ROW_TILE
    return [(0, first), (first, rows)]


def half_block(kept, given, devices, bound):
    kept, received = across_cores(kept, given, devices)
    chip = kept + received
    rows = kept.shape[0] // 4
    encode, decode = to_half(2.0 * bound)
    ranges = cuts(rows)
    received = [
        [swap(encode(chip[k * rows + low:k * rows + high]), devices, 2 * k) for k in range(1, 4)]
        for low, high in ranges
    ]
    done = []
    for (low, high), others in zip(ranges, received):
        total = four_sum(chip[low:high], [decode(other) for other in others])
        reach = 8.0 * bound
        bit = 8
        while bit < devices:
            encode_z, decode_z = to_half(reach)
            sent = encode_z(total)
            others = spread(sent, devices, bit)
            total = four_sum(decode_z(sent), [decode_z(other) for other in others])
            reach = reach * (len(others) + 1)
            bit = bit * (len(others) + 1)
        done.append(normalise(total))
    return done


def full_block(kept, given, devices):
    kept, received = across_cores(kept, given, devices)
    rows, samples = kept.shape[0] // 4, kept.shape[1]
    own = pltpu.VMEM((rows, samples), jnp.float32)
    coded = pltpu.VMEM((rows + ROW_TILE * words_for(rows // ROW_TILE), samples), jnp.int16)

    def call(kernel, out_shape, *operands):
        return pl.pallas_call(
            kernel,
            out_shape=out_shape,
            in_specs=in_vmem(len(operands)),
            out_specs=in_vmem(len(out_shape)),
            compiler_params=pltpu.CompilerParams(vmem_limit_bytes=KERNEL_BYTES),
        )(*[on_chip(operand) for operand in operands])

    total, *sent = call(encode_kernel, [own] + [coded] * 3, kept, received)
    others = [swap(sent[k - 1], devices, 2 * k) for k in range(1, 4)]
    bit = 8
    while bit < devices:
        total, sent = call(recode_kernel, [own, coded], total, *others)
        others = spread(sent, devices, bit)
        bit = bit * (len(others) + 1)
    return call(finish_kernel, [pltpu.VMEM((rows, samples), jnp.bfloat16)], total, *others)


def gather_blocks(pieces, devices):
    blocks = [[piece] + [swap(piece, devices, 2 * k) for k in range(1, 4)] for piece in pieces]
    half = jnp.concatenate([block[k] for k in range(4) for block in blocks], axis=0)
    return half, swap(half, devices, 1)


FIRST_CHUNKS = 2
LAST_CHUNKS = 2
KERNEL_BYTES = 24 << 20


def dot_tt(a, b):
    return lax.dot_general(a, b, (((1,), (1,)), ((), ())), preferred_element_type=jnp.float32)


def dot(a, b):
    return lax.dot_general(a, b, (((1,), (0,)), ((), ())), preferred_element_type=jnp.float32)


def slots(label, mine, rows):
    used = -(-MODULES // BLOCKS)
    block = jnp.zeros_like(label)
    for b in range(1, BLOCKS):
        block += jnp.where(label >= b * used, 1, 0)
    return (block ^ mine) * rows + (label - block * used)


def first_kernel(mine_ref, label_hbm, expression_ref, standard_ref, given_ref, buffer, label_ref, sems, label_sem):
    genes, samples = standard_ref.shape
    size = genes // FIRST_CHUNKS
    copies = [
        pltpu.make_async_copy(expression_ref.at[pl.ds(c * size, size)], buffer.at[pl.ds(c * size, size)], sems.at[c])
        for c in range(FIRST_CHUNKS)
    ]
    label_copy = pltpu.make_async_copy(label_hbm, label_ref, label_sem)
    label_copy.start()
    for copy in copies:
        copy.start()
    label_copy.wait()
    slot = slots(label_ref[...], mine_ref[0], given_ref.shape[0] // (BLOCKS // 2)) - given_ref.shape[0]
    for c, copy in enumerate(copies):
        copy.wait()
        span = pl.ds(c * size, size)
        values = buffer[span, :].astype(jnp.float32)
        centre = jnp.sum(values, axis=1, keepdims=True) * (1.0 / samples)
        shifted = values - centre
        spread = jnp.sum(shifted * shifted, axis=1, keepdims=True) * (1.0 / samples)
        part = (shifted * lax.rsqrt(spread + epsilon)).astype(jnp.bfloat16)
        standard_ref[span, :] = part
        row = lax.broadcasted_iota(jnp.int32, (given_ref.shape[0], size), 0)
        weights = jnp.where(row == slot[:, c * size:(c + 1) * size], 1.0, 0.0).astype(jnp.bfloat16)
        if c == 0:
            given_ref[...] = dot(weights, part)
        else:
            given_ref[...] += dot(weights, part)


def raise_half(eigengenes, standard, start, mine):
    samples = standard.shape[1]
    rows = eigengenes.shape[0] // (BLOCKS // 2)
    used = -(-MODULES // BLOCKS)
    row = jnp.arange(eigengenes.shape[0], dtype=jnp.int32)
    number = ((start + row // rows) ^ mine) * used + row % rows
    real = (row % rows < used) & (number < MODULES)
    raised = jnp.exp(dot_tt(standard, eigengenes) * (sharpness / samples))
    return jnp.where(real[None, :], raised, 0.0)


def weigh(weights, standard):
    return lax.dot_general(weights, standard, (((0,), (0,)), ((), ())), preferred_element_type=jnp.float32)


def last_kernel(source_ref, mine_ref, other_ref, standard_ref, share_ref, eigen_hbm, eigen_ref, sem):
    copy = pltpu.make_async_copy(eigen_ref, eigen_hbm, sem)

    @pl.when(pl.program_id(0) == 0)
    def _():
        half = mine_ref.shape[0]
        column = lax.broadcasted_iota(jnp.int32, (MODULES, half), 1)
        rows = source_ref[...]
        first = jnp.where(column == rows, 1.0, 0.0).astype(jnp.bfloat16)
        second = jnp.where(column == rows - half, 1.0, 0.0).astype(jnp.bfloat16)
        picked = dot(first, mine_ref[...]) + dot(second, other_ref[...])
        eigen_ref[...] = picked.astype(jnp.bfloat16)
        copy.start()

    genes, samples = standard_ref.shape
    size = genes // LAST_CHUNKS
    part = standard_ref[pl.ds(pl.multiple_of(pl.program_id(0) * size, size), size), :]
    raised = jnp.exp(dot_tt(eigen_ref[...], part) * (sharpness / samples))
    share_ref[...] = raised * (MODULES / jnp.sum(raised, axis=0, keepdims=True))

    @pl.when(pl.program_id(0) == LAST_CHUNKS - 1)
    def _():
        copy.wait()


def on_chip(value):
    return pltpu.with_memory_space_constraint(value, pltpu.VMEM)


def in_vmem(count):
    return [pl.BlockSpec(memory_space=pltpu.VMEM)] * count


def shards(devices):
    def body(expression, labels):
        return steps(expression, labels)

    def steps(expression, labels):
        genes, samples = expression.shape
        used = -(-MODULES // BLOCKS)
        rows = -(-used // ROW_TILE) * ROW_TILE
        half = BLOCKS // 2 * rows
        place = lax.axis_index(AXIS)
        mine = ((place & 1) * 4 + ((place >> 1) & 3)).astype(jnp.int32)
        bound = genes * math.sqrt(samples) * 1.02
        f32 = jnp.float32

        module = jnp.arange(MODULES, dtype=jnp.int32)
        source = (((module // used) ^ mine) * rows + module % used)[:, None]

        standard, given = pl.pallas_call(
            first_kernel,
            out_shape=[pltpu.VMEM((genes, samples), jnp.bfloat16), pltpu.VMEM((half, samples), f32)],
            in_specs=[
                pl.BlockSpec(memory_space=pltpu.SMEM),
                pl.BlockSpec(memory_space=pltpu.HBM),
                pl.BlockSpec(memory_space=pltpu.HBM),
            ],
            out_specs=in_vmem(2),
            scratch_shapes=[
                pltpu.VMEM((genes, samples), jnp.bfloat16),
                pltpu.VMEM((1, genes), jnp.int32),
                pltpu.SemaphoreType.DMA((FIRST_CHUNKS,)),
                pltpu.SemaphoreType.DMA,
            ],
            name="first",
                compiler_params=pltpu.CompilerParams(vmem_limit_bytes=KERNEL_BYTES),
        )(mine[None], pltpu.with_memory_space_constraint(labels[None, :], pltpu.HBM), pltpu.with_memory_space_constraint(expression, pltpu.HBM))
        slot = slots(labels, mine, rows)
        column = jnp.arange(half, dtype=jnp.int32)
        kept = weigh((slot[:, None] == column[None, :]).astype(jnp.bfloat16), standard)
        for iteration in range(ITERS):
            last = iteration == ITERS - 1
            block = half_block(kept, given, devices, bound) if last else full_block(kept, given, devices)
            own, other = gather_blocks(block, devices)
            if not last:
                mine_raised = raise_half(own, standard, 0, mine)
                other_raised = raise_half(other, standard, BLOCKS // 2, mine)
                total = jnp.sum(mine_raised, axis=1, keepdims=True) + jnp.sum(other_raised, axis=1, keepdims=True)
                given = weigh((other_raised / total).astype(jnp.bfloat16), standard)
                kept = weigh((mine_raised / total).astype(jnp.bfloat16), standard)
        size = genes // LAST_CHUNKS
        shares, eigengenes = pl.pallas_call(
            last_kernel,
            out_shape=[
                jax.ShapeDtypeStruct((MODULES, genes), f32),
                jax.ShapeDtypeStruct((MODULES, samples), jnp.bfloat16),
            ],
            grid=(LAST_CHUNKS,),
            in_specs=[
                pl.BlockSpec((MODULES, 1), lambda c: (0, 0)),
            ] + in_vmem(3),
            out_specs=[
                pl.BlockSpec((MODULES, size), lambda c: (0, c)),
                pl.BlockSpec(memory_space=pltpu.HBM),
            ],
            scratch_shapes=[pltpu.VMEM((MODULES, samples), jnp.bfloat16), pltpu.SemaphoreType.DMA],
            name="last",
                compiler_params=pltpu.CompilerParams(vmem_limit_bytes=KERNEL_BYTES),
        )(source, on_chip(own), on_chip(other), on_chip(standard))
        return shares.T, eigengenes

    return body


def solution(mesh):
    placed = (P(AXIS, None), P(AXIS))
    return jax.shard_map(
        shards(mesh.shape[AXIS]), mesh=mesh, in_specs=placed, out_specs=(P(AXIS, None), P()), check_vma=False
    )
```
